32 devices in a mesh: grp: 2 (over y), kvp: 4 (over z), tp: 4 (over x, core).
Axes of the slice: x: 2, y: 2, z: 4, core: 2. Of those that a mesh axis runs over, the one named last changes fastest.
Arguments:
- queries: bfloat16 [32, 4096], P('grp', 'tp'), parts along dimension 0, may hold values from -6 to 6
- keys: bfloat16 [32, 512, 512], P('grp', 'kvp', 'tp'), parts along dimension 0, may hold values from -6 to 6
- values: bfloat16 [32, 512, 512], P('grp', 'kvp', 'tp'), parts along dimension 0, may hold values from -6 to 6
- lengths: int32 [32], P('grp'), parts along dimension 0, may hold values from 256 to 512, as said below
- out_weight: bfloat16 [4096, 1536], P('tp', 'kvp'), may hold values from -0.375 to 0.375
- residual: bfloat16 [32, 1536], P('grp', 'kvp'), parts along dimension 0, may hold values from -20 to 20
- norm_gain: bfloat16 [1536], P('kvp'), may hold values from 0.099609375 to 1.8984375
- expert_ids: int32 [32, 4], P('grp'), parts along dimension 0, may hold values from 0 to 3, as said below
- gate_probs: float32 [32, 4], P('grp'), parts along dimension 0, may hold values from 0.2 to 1
- w_gate: bfloat16 [4, 1536, 1536], P('kvp', None, 'tp'), may hold values from -0.15625 to 0.15625
- w_up: bfloat16 [4, 1536, 1536], P('kvp', None, 'tp'), may hold values from -0.15625 to 0.15625
- w_down: bfloat16 [4, 1536, 1536], P('kvp', 'tp'), may hold values from -0.15625 to 0.15625
Outputs:
- attended: float32 [32, 4096], P('grp', 'tp'), parts along dimension 0
- mixed: bfloat16 [32, 1536], P('grp', 'kvp'), parts along dimension 0
The draws below stay inside these ranges and needn't reach their ends.
There are 2 independent parts, one for each index of `grp`. The reference program is written for one: setup_inputs(seed, part) draws one part's arguments, and reference() takes and returns one part's arrays. A program takes and returns all parts, laid end to end along the dimension named above; an argument that names none is the same for every part. Nothing has to cross between parts.
Inputs may be any that keep to these rules, and one draw needn't show every extreme that they name: `lengths`: at least one sequence has all 512 positions valid. `expert_ids`: each row names 4 different experts; no expert is named by more than 16 rows, and some expert by exactly 16.
All inputs are finite; a program needn't handle non-finite values.
Results may differ from the reference program's by a relative error of at most 0.006.
Values may be sent and summed in bfloat16 or wider, within the bound.
No kernel may reach another device: no remote copies, remote signals or barrier semaphores. Data moves between devices by JAX's collectives and lax.ppermute only.
A program may use at most 64 MiB of HBM per device.

```python
import math
import jax
import jax.numpy as jnp
from jax import lax

D = 1536
FF = 1536
HEADS = 64
KV_HEADS = 8
HEAD = 64
TOP = 4
EXP_DEV = 1
BATCH = 16
CTX_DEV = 128
EXPERTS = 4
CONTEXT = 512
CAP = 16
N_KVP = 4


def draw_queries(key, part):
    base_draw = jnp.clip(jax.random.normal(jax.random.fold_in(key, 42), (BATCH, HEADS * HEAD), jnp.float32), -4.5, 4.5)
    return base_draw.astype(jnp.bfloat16)


def draw_keys(key, part):
    context = CTX_DEV * N_KVP
    base_draw = jnp.clip(jax.random.normal(jax.random.fold_in(key, 44), (BATCH, context, KV_HEADS * HEAD), jnp.float32), -4.5, 4.5)
    return base_draw.astype(jnp.bfloat16)


def draw_lengths(key, part):
    context = CTX_DEV * N_KVP
    drawn_len = jax.random.randint(jax.random.fold_in(key, 11), (BATCH,), 2 * CTX_DEV, context + 1)
    full_row = jax.random.randint(jax.random.fold_in(key, 12), (), 0, BATCH)
    return jnp.where(jnp.arange(BATCH) == full_row, context, drawn_len).astype(jnp.int32)


def draw_expert_ids(key, part):
    experts = EXP_DEV * N_KVP
    least_group = min(CAP, (BATCH * TOP + experts - 1) // experts)
    sizes_drawn = jax.random.randint(jax.random.fold_in(key, 21), (TOP,), least_group, CAP + 1)
    sizes_drawn = sizes_drawn.at[0].set(CAP)
    span_size = (BATCH + sizes_drawn - 1) // sizes_drawn
    offsets = jnp.cumsum(span_size) - span_size
    row_keys = jax.random.split(jax.random.fold_in(key, 22), TOP)

    def shuffle(subkey):
        return jax.random.permutation(subkey, BATCH)
    orders = jax.vmap(shuffle)(row_keys)
    slot_ids = offsets[:, None] + orders // sizes_drawn[:, None]
    labels = jax.random.permutation(jax.random.fold_in(key, 23), experts)
    return labels[slot_ids].T.astype(jnp.int32)


def draw_residual(key, part):
    rising = jnp.exp(jnp.linspace(math.log(0.5), math.log(1.5), D))
    columns = rising * jnp.exp(jax.random.uniform(jax.random.fold_in(key, 51), (D,), jnp.float32, math.log(0.6), math.log(2.0)))
    row_scale = jnp.exp(jax.random.uniform(jax.random.fold_in(key, 55), (BATCH, 1), jnp.float32, math.log(0.5), math.log(2.0)))
    base_draw = jnp.clip(jax.random.normal(jax.random.fold_in(key, 56), (BATCH, D), jnp.float32), -3.0, 3.0)
    return (base_draw * row_scale * columns[None, :]).astype(jnp.bfloat16)


def shard_levels(own_key, shape, cuts, smallest, largest):
    gain = 1.0
    for dim, parts in cuts:
        draws = jax.random.uniform(jax.random.fold_in(jax.random.fold_in(own_key, 6), dim), (parts,), jnp.float32, smallest / len(cuts), largest / len(cuts))
        gain = gain * jnp.repeat(jnp.exp(draws), shape[dim] // parts).reshape((-1,) + (1,) * (len(shape) - 1 - dim))
    return gain


def centred(stream_key, extent, scale, bound, cuts=(), kind=jnp.bfloat16):
    entries = scale * jax.random.normal(stream_key, extent, jnp.float32)
    if cuts:
        entries = entries * shard_levels(stream_key, extent, cuts, -0.22, 0.18)
    return jnp.clip(entries, -bound, bound).astype(kind)


def setup_inputs(seed: int = 0, part: int = 0) -> dict:
    streams_of = jax.random.split(jax.random.key(seed), 13)
    part_splits = jax.random.split(jax.random.fold_in(streams_of[12], part), 13)
    queries = draw_queries(jax.random.fold_in(jax.random.fold_in(streams_of[12], part), 71), part)
    keys = draw_keys(jax.random.fold_in(jax.random.fold_in(streams_of[12], part), 71), part)
    values = centred(part_splits[2], (BATCH, CONTEXT, KV_HEADS * HEAD), 1.0, 6.0, ((1, 4), (2, 4)))
    lengths = draw_lengths(jax.random.fold_in(jax.random.fold_in(streams_of[12], part), 71), part)
    out_weight = centred(streams_of[4], (HEADS * HEAD, D), (4 * HEAD) ** -0.5, 0.375, ((0, 4), (1, 4)))
    residual = draw_residual(jax.random.fold_in(jax.random.fold_in(streams_of[12], part), 71), part)
    norm_gain = jnp.clip(1.0 + 0.18 * jax.random.normal(streams_of[6], (D,), jnp.float32), 0.099609375, 1.8984375).astype(jnp.bfloat16)
    expert_ids = draw_expert_ids(jax.random.fold_in(jax.random.fold_in(streams_of[12], part), 71), part)
    gate_probs = jnp.clip(jax.random.uniform(part_splits[8], (BATCH, TOP), jnp.float32, 0.2, 1.0), 0.2, 1.0)
    w_gate = centred(streams_of[9], (EXPERTS, D, FF), D ** -0.5, 0.15625, ((0, 4), (2, 4)))
    w_up = centred(streams_of[10], (EXPERTS, D, FF), D ** -0.5, 0.15625, ((0, 4), (2, 4)))
    w_down = centred(streams_of[11], (EXPERTS, FF, D), FF ** -0.5, 0.15625, ((0, 4), (1, 4)))
    return {"queries": queries, "keys": keys, "values": values, "lengths": lengths, "out_weight": out_weight, "residual": residual, "norm_gain": norm_gain, "expert_ids": expert_ids, "gate_probs": gate_probs, "w_gate": w_gate, "w_up": w_up, "w_down": w_down}


EPSILON = 1e-05
NEGATIVE = -1e+30

def slot_tables(expert_ids, gate_probs, experts, capacity):
    batch_size, top_count = expert_ids.shape
    flat_ids = expert_ids.reshape(-1)
    pair_count = flat_ids.shape[0]
    pair_order = jnp.arange(pair_count, dtype=jnp.int32)
    earlier_same = (flat_ids[:, None] == flat_ids[None, :]) & (pair_order[None, :] < pair_order[:, None])
    slot_index = lax.optimization_barrier(jnp.sum(earlier_same.astype(jnp.int32), axis=1))
    target_col = flat_ids * capacity + slot_index
    columns = jnp.arange(experts * capacity, dtype=jnp.int32)
    hit_table = (target_col[:, None] == columns[None, :]).astype(jnp.float32)
    hit_table = hit_table.reshape(batch_size, top_count, experts * capacity)
    dispatch = lax.optimization_barrier(jnp.sum(hit_table, axis=1))
    combine = lax.optimization_barrier(jnp.sum(hit_table * gate_probs[:, :, None], axis=1))
    return (dispatch, combine)

def run_expert(operands):
    expert_rows, gate_w, up_w, down_w = operands
    gate_proj = jnp.dot(expert_rows, gate_w, preferred_element_type=jnp.float32)
    up_proj = jnp.dot(expert_rows, up_w, preferred_element_type=jnp.float32)
    activation = (jax.nn.silu(gate_proj) * up_proj).astype(jnp.bfloat16)
    return jnp.dot(activation, down_w, preferred_element_type=jnp.float32)

def reference(queries, keys, values, lengths, out_weight, residual, norm_gain, expert_ids, gate_probs, w_gate, w_up, w_down):
    batch_size = queries.shape[0]
    group_size = HEADS // KV_HEADS
    query_heads = queries.astype(jnp.float32).reshape(batch_size, KV_HEADS, group_size, HEAD)
    key_blocks = keys.astype(jnp.float32).reshape(batch_size, N_KVP, CTX_DEV, KV_HEADS, HEAD)
    value_blocks = values.astype(jnp.float32).reshape(batch_size, N_KVP, CTX_DEV, KV_HEADS, HEAD)
    scores = jnp.einsum('bgrd,bncgd->bgrnc', query_heads, key_blocks) * HEAD ** (-0.5)
    position = jnp.arange(N_KVP * CTX_DEV, dtype=jnp.int32).reshape(N_KVP, CTX_DEV)
    valid_key = (position[None] < lengths[:, None, None])[:, None, None]
    masked = jnp.where(valid_key, scores, NEGATIVE)
    block_max = lax.optimization_barrier(jnp.max(masked, axis=4))
    weights = jnp.where(valid_key, jnp.exp(masked - block_max[..., None]), 0.0)
    rounded = lax.optimization_barrier(weights.astype(jnp.bfloat16)).astype(jnp.float32)
    block_sum = lax.optimization_barrier(jnp.sum(rounded, axis=4))
    block_out = jnp.einsum('bgrnc,bncgd->bgrnd', rounded, value_blocks)
    global_max = lax.optimization_barrier(jnp.max(block_max, axis=3))
    rescale = jnp.exp(block_max - global_max[..., None])
    denominator = lax.optimization_barrier(jnp.sum(rescale * block_sum, axis=3))
    attended = lax.optimization_barrier(jnp.sum(rescale[..., None] * block_out, axis=3)) / denominator[..., None]
    attended = attended.reshape(batch_size, HEADS * HEAD)
    projected = jnp.dot(attended.astype(jnp.bfloat16), out_weight, preferred_element_type=jnp.float32)
    hidden_state = lax.optimization_barrier((projected + residual.astype(jnp.float32)).astype(jnp.bfloat16))
    state_wide = hidden_state.astype(jnp.float32)
    mean_square = lax.optimization_barrier(jnp.sum(state_wide * state_wide, axis=1)) / D
    normed = (state_wide * lax.rsqrt(mean_square + EPSILON)[:, None] * norm_gain.astype(jnp.float32)[None, :]).astype(jnp.bfloat16)
    dispatch, combine = slot_tables(expert_ids, gate_probs, EXPERTS, CAP)
    expert_rows = jnp.dot(dispatch.T.astype(jnp.bfloat16), normed, preferred_element_type=jnp.float32).astype(jnp.bfloat16)
    expert_rows = expert_rows.reshape(EXPERTS, CAP, D)
    expert_out = lax.map(run_expert, (expert_rows, w_gate, w_up, w_down))
    moe_term = jnp.dot(combine, expert_out.reshape(EXPERTS * CAP, D), precision=lax.Precision.HIGHEST)
    mixed = (state_wide + moe_term).astype(jnp.bfloat16)
    return (attended, mixed)
```

```python
import functools

import jax
import jax.numpy as jnp
from jax import lax
from jax.experimental import pallas as pl
from jax.experimental.pallas import tpu as pltpu
from jax.sharding import PartitionSpec as P

HEAD = 64
LANES = 128
EPSILON = 1e-05
NEGATIVE = -1e30
F32 = jnp.float32
BF16 = jnp.bfloat16
VMEM = pl.BlockSpec(memory_space=pltpu.VMEM)
SMEM = pl.BlockSpec(memory_space=pltpu.SMEM)
ANY = pl.BlockSpec(memory_space=pl.ANY)


def exchange(x, axis):
    size = lax.axis_size(axis)
    moved = [lax.ppermute(x, axis, [(i, i ^ s) for i in range(size)]) for s in range(size - 1, 0, -1)]
    return [x] + moved[::-1]


def pairwise(parts, add):
    parts = list(parts)
    while len(parts) > 1:
        parts = [add(parts[i], parts[i + 1]) for i in range(0, len(parts), 2)]
    return parts[0]


def add(a, b):
    return a + b


def split3(x):
    first = x.astype(BF16).astype(F32)
    rest = x - first
    second = rest.astype(BF16).astype(F32)
    return first, second, (rest - second).astype(BF16).astype(F32)


def attention_body(heads, kv, chunks, len_ref, q_ref, k_hbm, v_hbm, out_ref, k_buf, v_buf, rows, stats, sems):
    batch, context = k_buf.shape[:2]
    group = heads // kv
    step = batch // chunks

    def copy(source, target, which, c):
        part = pl.ds(c * step, step)
        return pltpu.make_async_copy(source.at[part], target.at[part], sems.at[which, c])

    for c in range(chunks):
        copy(k_hbm, k_buf, 0, c).start()
    for c in range(chunks):
        copy(v_hbm, v_buf, 1, c).start()
    lane = lax.broadcasted_iota(jnp.int32, (batch, LANES), 1)
    low = lane < HEAD
    for h in range(heads):
        wide = q_ref[:, (h // 2) * LANES : (h // 2 + 1) * LANES].astype(F32)
        half = h // group
        if h % 2 != half:
            wide = pltpu.roll(wide, HEAD, 1)
        rows[h * batch : (h + 1) * batch, :] = jnp.where(low if half == 0 else ~low, wide, 0.0)
    base = lax.axis_index("kvp") * context
    spot = lax.broadcasted_iota(jnp.int32, (heads, context), 1)
    slot = lax.broadcasted_iota(jnp.int32, (heads, LANES), 1)
    mine = slot % heads == lax.broadcasted_iota(jnp.int32, (heads, LANES), 0)
    field = slot // heads
    query = [rows[pl.ds(b, heads, stride=batch), :].astype(BF16) for b in range(batch)]
    for b in range(batch):
        if b % step == 0:
            copy(k_hbm, k_buf, 0, b // step).wait()
            copy(v_hbm, v_buf, 1, b // step).wait()
        scores = lax.dot_general(
            query[b], k_buf[b], (((1,), (1,)), ((), ())), preferred_element_type=F32
        ) * HEAD ** (-0.5)
        valid = spot < len_ref[b] - base
        masked = jnp.where(valid, scores, NEGATIVE)
        top = jnp.max(masked, axis=1, keepdims=True)
        weights = jnp.where(valid, jnp.exp(masked - top), 0.0).astype(BF16)
        total = jnp.sum(weights.astype(F32), axis=1, keepdims=True)
        summed = jnp.dot(weights, v_buf[b], preferred_element_type=F32)
        rows[b * heads : (b + 1) * heads, :] = jnp.where(total > 0.0, summed / jnp.where(total > 0.0, total, 1.0), 0.0)
        value = jnp.zeros((heads, LANES), F32)
        for i, term in enumerate(split3(top) + split3(total)):
            value = jnp.where(mine & (field == i), jnp.broadcast_to(term, (heads, LANES)), value)
        stats[b : b + 1, :] = jnp.sum(value, axis=0, keepdims=True)
    for pair in range(heads // 2):
        sides = []
        for h in (2 * pair, 2 * pair + 1):
            wide = rows[pl.ds(h, batch, stride=heads), :]
            sides.append(pltpu.roll(wide, HEAD, 1) if h % 2 != h // group else wide)
        out_ref[:, pair * LANES : (pair + 1) * LANES] = jnp.where(low, sides[0], sides[1]).astype(BF16)
    out_ref[:, heads * HEAD :] = stats[...].astype(BF16)


def attention(queries, keys, values, lengths):
    batch, context, width = keys.shape
    heads = queries.shape[1] // HEAD
    chunks = 4
    return pl.pallas_call(
        functools.partial(attention_body, heads, width // HEAD, chunks),
        out_shape=jax.ShapeDtypeStruct((batch, heads * HEAD + LANES), BF16),
        in_specs=[SMEM, VMEM, ANY, ANY],
        out_specs=VMEM,
        scratch_shapes=[
            pltpu.VMEM(keys.shape, BF16),
            pltpu.VMEM(values.shape, BF16),
            pltpu.VMEM((batch * heads, LANES), F32),
            pltpu.VMEM((batch, LANES), F32),
            pltpu.SemaphoreType.DMA((2, chunks)),
        ],
        name="attention",
    )(lengths, queries, keys, values)


def merge_body(heads, size, *refs):
    parts, weight, attended_ref, out_ref = refs[:size], refs[size], refs[size + 1], refs[size + 2]
    batch = parts[0].shape[0]
    tops, totals = [], []
    for part in parts:
        stats = part[:, heads * HEAD :].astype(F32)
        turned = [stats] + [pltpu.roll(stats, LANES - i * heads, 1) for i in range(1, 6)]
        tops.append(turned[0] + turned[1] + turned[2])
        totals.append(turned[3] + turned[4] + turned[5])
    top = pairwise(tops, jnp.maximum)
    shares = [jnp.exp(t - top) * s for t, s in zip(tops, totals)]
    inverse = 1.0 / pairwise(shares, add)
    shares = [s * inverse for s in shares]
    low = lax.broadcasted_iota(jnp.int32, (batch, LANES), 1) < HEAD
    wide = (batch, LANES)
    pieces = []
    for pair in range(heads // 2):
        columns = slice(pair * LANES, (pair + 1) * LANES)
        terms = []
        for share, part in zip(shares, parts):
            left = jnp.broadcast_to(share[:, 2 * pair : 2 * pair + 1], wide)
            right = jnp.broadcast_to(share[:, 2 * pair + 1 : 2 * pair + 2], wide)
            terms.append(jnp.where(low, left, right) * part[:, columns].astype(F32))
        piece = pairwise(terms, add)
        attended_ref[:, columns] = piece
        pieces.append(piece.astype(BF16))
    out_ref[...] = jnp.dot(jnp.concatenate(pieces, axis=1), weight[...], preferred_element_type=F32).astype(BF16)


def merge(parts, weight):
    batch = parts[0].shape[0]
    inputs, columns = weight.shape
    return pl.pallas_call(
        functools.partial(merge_body, inputs // HEAD, len(parts)),
        out_shape=(
            jax.ShapeDtypeStruct((batch, inputs), F32),
            jax.ShapeDtypeStruct((batch, columns), BF16),
        ),
        in_specs=[VMEM] * (len(parts) + 1),
        out_specs=(VMEM, VMEM),
        name="merge",
    )(*parts, weight)


def state_body(size, *refs):
    parts, residual, gain, state_ref, out_ref = refs[:size], *refs[size:]
    projected = pairwise([p[...].astype(F32) for p in parts], add)
    state = (projected + residual[...].astype(F32)).astype(BF16)
    state_ref[...] = state
    state = state.astype(F32)
    columns = state.shape[1]
    out_ref[:, :columns] = (state * gain[...].astype(F32)).astype(BF16)
    squares = jnp.sum(state * state, axis=1, keepdims=True)
    lane = lax.broadcasted_iota(jnp.int32, (state.shape[0], LANES), 1)
    value = jnp.zeros(lane.shape, F32)
    for i, term in enumerate(split3(squares)):
        value = jnp.where(lane == i, jnp.broadcast_to(term, lane.shape), value)
    out_ref[:, columns:] = value.astype(BF16)


def state(parts, residual, gain):
    batch, columns = residual.shape
    return pl.pallas_call(
        functools.partial(state_body, len(parts)),
        out_shape=(
            jax.ShapeDtypeStruct((batch, columns), BF16),
            jax.ShapeDtypeStruct((batch, columns + LANES), BF16),
        ),
        in_specs=[VMEM] * (len(parts) + 2),
        out_specs=(VMEM, VMEM),
        name="state",
    )(*parts, residual, gain)


def expert_body(size, *refs):
    parts, (ids, probs, gate, up, down), outs = refs[:size], refs[size : size + 5], refs[size + 5 :]
    columns = outs[0].shape[1]
    me = lax.axis_index("kvp")
    held = gate.shape[0]
    squares = pairwise([jnp.sum(p[:, columns:].astype(F32), axis=1, keepdims=True) for p in parts], add)
    inverse = lax.rsqrt(squares / (columns * size) + EPSILON)
    sums = [0.0] * size
    for e in range(held):
        gate_sum, up_sum = 0.0, 0.0
        for s in range(size):
            rows = pl.ds(pl.multiple_of((me ^ s) * columns, LANES), columns)
            block = parts[s][:, :columns]
            gate_sum += jnp.dot(block, gate[e, rows, :], preferred_element_type=F32)
            up_sum += jnp.dot(block, up[e, rows, :], preferred_element_type=F32)
        gate_sum, up_sum = gate_sum * inverse, up_sum * inverse
        hidden = (gate_sum / (1.0 + jnp.exp(-gate_sum)) * up_sum).astype(BF16)
        chosen = ids[...] == me * held + e
        scale = jnp.sum(jnp.where(chosen, probs[...], 0.0), axis=1, keepdims=True)
        for s in range(size):
            target = pl.ds(pl.multiple_of((me ^ s) * columns, LANES), columns)
            sums[s] += jnp.dot(hidden, down[e, :, target], preferred_element_type=F32) * scale
    for s in range(size):
        outs[s][...] = sums[s].astype(BF16)


def experts(parts, ids, probs, gate, up, down):
    size = len(parts)
    batch = parts[0].shape[0]
    columns = parts[0].shape[1] - LANES
    return pl.pallas_call(
        functools.partial(expert_body, size),
        out_shape=tuple(jax.ShapeDtypeStruct((batch, columns), BF16) for _ in range(size)),
        in_specs=[VMEM] * (size + 5),
        out_specs=(VMEM,) * size,
        name="experts",
    )(*parts, ids, probs, gate, up, down)


def small_slice(
    queries, keys, values, lengths, out_weight, residual, norm_gain, expert_ids, gate_probs, w_gate, w_up, w_down
):
    parts = exchange(attention(queries, keys, values, lengths), "kvp")
    attended, projected = merge(parts, out_weight)
    own_state, message = state(exchange(projected, "tp"), residual, norm_gain.reshape(1, -1))
    outputs = experts(exchange(message, "kvp"), expert_ids, gate_probs, w_gate, w_up, w_down)
    size = len(outputs)
    moved = [outputs[0]] + [
        lax.ppermute(outputs[s], "kvp", [(i, i ^ s) for i in range(size)]) for s in range(1, size)
    ]
    owned = pairwise([m.astype(F32) for m in moved], add).astype(BF16)
    moe_term = pairwise([m.astype(F32) for m in exchange(owned, "tp")], add)
    return attended, (own_state.astype(F32) + moe_term).astype(BF16)


def merged(part, axis, combine):
    gathered = jax.tree.map(lambda a: lax.all_gather(a, axis), part)

    def take(source):
        return jax.tree.map(lambda a: lax.dynamic_index_in_dim(a, source, 0, False), gathered)

    return lax.fori_loop(
        1, lax.axis_size(axis), lambda source, state: combine(state, take(source)), take(0)
    )


def slot_tables(expert_ids, gate_probs, experts, capacity):
    batch_size, top_count = expert_ids.shape
    flat_ids = expert_ids.reshape(-1)
    pair_count = flat_ids.shape[0]
    pair_order = jnp.arange(pair_count, dtype=jnp.int32)
    earlier_same = (flat_ids[:, None] == flat_ids[None, :]) & (
        pair_order[None, :] < pair_order[:, None]
    )
    slot_index = jnp.sum(earlier_same.astype(jnp.int32), axis=1)
    target_col = flat_ids * capacity + slot_index
    columns = jnp.arange(experts * capacity, dtype=jnp.int32)
    hit_table = (target_col[:, None] == columns[None, :]).astype(jnp.float32)
    hit_table = hit_table.reshape(batch_size, top_count, experts * capacity)
    dispatch = jnp.sum(hit_table, axis=1)
    combine = jnp.sum(hit_table * gate_probs[:, :, None], axis=1)
    return (dispatch, combine)


def merge_partial(earlier, latest):
    global_max = jnp.maximum(earlier[0], latest[0])
    lead_scale = jnp.exp(earlier[0] - global_max)
    trail_scale = jnp.exp(latest[0] - global_max)
    return (
        global_max,
        lead_scale * earlier[1] + trail_scale * latest[1],
        lead_scale[..., None] * earlier[2] + trail_scale[..., None] * latest[2],
    )


def large_slice(
    queries,
    keys,
    values,
    lengths,
    out_weight,
    residual,
    norm_gain,
    expert_ids,
    gate_probs,
    w_gate,
    w_up,
    w_down,
):
    batch_size = queries.shape[0]
    local_kv = keys.shape[2] // HEAD
    local_heads = queries.shape[1] // HEAD
    group_size = local_heads // local_kv
    ctx_dev = keys.shape[1]
    shards = lax.axis_size("kvp")
    query_heads = queries.reshape(batch_size, local_kv, group_size, HEAD)
    key_rows = keys.reshape(batch_size, ctx_dev, local_kv, HEAD)
    value_rows = values.reshape(batch_size, ctx_dev, local_kv, HEAD)
    scores = jnp.einsum(
        "bgrd,bcgd->bgrc", query_heads, key_rows, preferred_element_type=jnp.float32
    ) * HEAD ** (-0.5)
    position = lax.axis_index("kvp") * ctx_dev + jnp.arange(ctx_dev, dtype=jnp.int32)
    valid_key = (position[None, :] < lengths[:, None])[:, None, None, :]
    masked = jnp.where(valid_key, scores, NEGATIVE)
    block_max = jnp.max(masked, axis=3)
    weights = jnp.where(valid_key, jnp.exp(masked - block_max[..., None]), 0.0)
    rounded = weights.astype(jnp.bfloat16)
    block_sum = jnp.sum(rounded.astype(jnp.float32), axis=3)
    block_out = jnp.einsum(
        "bgrc,bcgd->bgrd", rounded, value_rows, preferred_element_type=jnp.float32
    )
    global_max, denominator, summed = merged(
        (block_max, block_sum, block_out), "kvp", merge_partial
    )
    attended = (summed / denominator[..., None]).reshape(batch_size, local_heads * HEAD)
    projected = lax.psum(
        jnp.dot(attended.astype(jnp.bfloat16), out_weight, preferred_element_type=jnp.float32), "tp"
    )
    hidden_state = lax.optimization_barrier(
        (projected + residual.astype(jnp.float32)).astype(jnp.bfloat16)
    )
    state_wide = hidden_state.astype(jnp.float32)
    col_count = hidden_state.shape[1]
    exp_dev = w_gate.shape[0]
    experts = exp_dev * shards
    capacity = min(batch_size, max(2, 2 * batch_size * expert_ids.shape[1] // experts))
    dispatch, combine = slot_tables(expert_ids, gate_probs, experts, capacity)
    total_sq = lax.psum(jnp.sum(state_wide * state_wide, axis=1), "kvp")
    inverse = lax.rsqrt(total_sq / (col_count * shards) + EPSILON)
    normed = (state_wide * inverse[:, None] * norm_gain.astype(jnp.float32)[None, :]).astype(
        jnp.bfloat16
    )
    outgoing = jnp.dot(
        dispatch.T.astype(jnp.bfloat16), normed, preferred_element_type=jnp.float32
    ).astype(jnp.bfloat16)
    outgoing = outgoing.reshape(experts, capacity, col_count)
    expert_rows = lax.all_to_all(outgoing, "kvp", split_axis=0, concat_axis=2, tiled=True)
    gate_proj = jnp.einsum("ecd,edf->ecf", expert_rows, w_gate, preferred_element_type=jnp.float32)
    up_proj = jnp.einsum("ecd,edf->ecf", expert_rows, w_up, preferred_element_type=jnp.float32)
    activation = (jax.nn.silu(gate_proj) * up_proj).astype(jnp.bfloat16)
    partial_value = jnp.einsum(
        "ecf,efd->ecd", activation, w_down, preferred_element_type=jnp.float32
    )
    returned = lax.all_to_all(partial_value, "kvp", split_axis=2, concat_axis=0, tiled=True)
    moe_local = jnp.dot(
        combine, returned.reshape(experts * capacity, col_count), precision=lax.Precision.HIGHEST
    )
    moe_term = lax.psum(moe_local, "tp")
    mixed = (state_wide + moe_term).astype(jnp.bfloat16)
    return (attended, mixed)


def on_device(queries, keys, values, lengths, out_weight, *rest):
    size, heads, kv = lax.axis_size("kvp"), queries.shape[1] // HEAD, keys.shape[2] // HEAD
    direct = (
        size in (2, 4, 8)
        and lax.axis_size("tp") in (2, 4, 8)
        and out_weight.shape[1] % LANES == 0
        and kv == 2
        and heads == 8 * kv
        and keys.shape[1] % LANES == 0
        and queries.shape[0] == 16
    )
    return (small_slice if direct else large_slice)(queries, keys, values, lengths, out_weight, *rest)


def solution(mesh):
    return jax.shard_map(
        on_device,
        mesh=mesh,
        in_specs=(
            P("grp", "tp"),
            P("grp", "kvp", "tp"),
            P("grp", "kvp", "tp"),
            P("grp"),
            P("tp", "kvp"),
            P("grp", "kvp"),
            P("kvp"),
            P("grp", None),
            P("grp", None),
            P("kvp", None, "tp"),
            P("kvp", None, "tp"),
            P("kvp", "tp", None),
        ),
        out_specs=(P("grp", "tp"), P("grp", "kvp")),
        check_vma=False,
    )
```

```python
import functools

import jax
import jax.numpy as jnp
from jax import lax
from jax.experimental import pallas as pl
from jax.experimental.pallas import tpu as pltpu
from jax.sharding import PartitionSpec as P


HEAD = 64
LANES = 128
EPSILON = 1e-05
NEGATIVE = -1e30
F32 = jnp.float32
BF16 = jnp.bfloat16
LIMIT = pltpu.CompilerParams(vmem_limit_bytes=8 * 1024 * 1024)
VMEM = pl.BlockSpec(memory_space=pltpu.VMEM)
HBM = pl.BlockSpec(memory_space=pltpu.HBM)


def turn(x, axis, s):
    return lax.ppermute(x, axis, [(i, i ^ s) for i in range(lax.axis_size(axis))])


def exchange(blocks, axis):
    moved = {s: turn(blocks[s], axis, s) for s in range(len(blocks) - 1, 0, -1)}
    return [blocks[0]] + [moved[s] for s in range(1, len(blocks))]


def share(x, axis):
    return exchange([x] * lax.axis_size(axis), axis)


def on_chip(x):
    return pltpu.with_memory_space_constraint(x, pltpu.VMEM)


def off_chip(x):
    return pltpu.with_memory_space_constraint(x, pltpu.HBM)


def pairwise(parts, add):
    parts = list(parts)
    while len(parts) > 1:
        parts = [add(parts[i], parts[i + 1]) for i in range(0, len(parts), 2)]
    return parts[0]


def add(a, b):
    return a + b


def split3(x):
    first = x.astype(BF16).astype(F32)
    rest = x - first
    second = rest.astype(BF16).astype(F32)
    return first, second, (rest - second).astype(BF16).astype(F32)


def attention_body(heads, kv, held, *refs):
    len_hbm, q_hbm, k_hbm, v_hbm = refs[:4]
    sources, out_ref, targets = refs[4 : 4 + held], refs[4 + held], refs[5 + held : 5 + 2 * held]
    lengths, q_buf, k_buf, v_buf, rows, sems = refs[5 + 2 * held :]
    batch, context = k_buf.shape[:2]
    group = heads // kv
    pairs = ((q_hbm, q_buf), (k_hbm, k_buf), (len_hbm, lengths), (v_hbm, v_buf)) + tuple(zip(sources, targets))
    copies = [pltpu.make_async_copy(source, target, sems.at[i]) for i, (source, target) in enumerate(pairs)]
    for c in copies:
        c.start()
    low = lax.broadcasted_iota(jnp.int32, (batch, LANES), 1) < HEAD
    spot = lax.broadcasted_iota(jnp.int32, (heads, context), 1) + lax.axis_index("kvp") * context
    copies[0].wait()
    for h in range(heads):
        wide = q_buf[:, (h // 2) * LANES : (h // 2 + 1) * LANES].astype(F32)
        half = h // group
        if h % 2 != half:
            wide = pltpu.roll(wide, HEAD, 1)
        rows[h * batch : (h + 1) * batch, :] = jnp.where(low if half == 0 else ~low, wide, 0.0)
    query = [rows[pl.ds(b, heads, stride=batch), :].astype(BF16) for b in range(batch)]
    copies[1].wait()
    scores = [
        lax.dot_general(query[b], k_buf[b], (((1,), (1,)), ((), ())), preferred_element_type=F32)
        for b in range(batch)
    ]
    copies[2].wait()
    valid = [spot < lengths[b] for b in range(batch)]
    masked = [jnp.where(valid[b], scores[b] * HEAD ** (-0.5), NEGATIVE) for b in range(batch)]
    top = [jnp.max(masked[b], axis=1, keepdims=True) for b in range(batch)]
    weights = [
        jnp.where(valid[b], jnp.exp(masked[b] - top[b]), 0.0).astype(BF16) for b in range(batch)
    ]
    total = [jnp.sum(weights[b].astype(F32), axis=1, keepdims=True) for b in range(batch)]
    copies[3].wait()
    summed = [jnp.dot(weights[b], v_buf[b], preferred_element_type=F32) for b in range(batch)]
    for b in range(batch):
        some = total[b] > 0.0
        rows[b * heads : (b + 1) * heads, :] = summed[b] * jnp.where(some, 1.0 / jnp.where(some, total[b], 1.0), 0.0)
    for pair in range(heads // 2):
        sides = []
        for h in (2 * pair, 2 * pair + 1):
            wide = rows[pl.ds(h, batch, stride=heads), :]
            sides.append(pltpu.roll(wide, HEAD, 1) if h % 2 != h // group else wide)
        out_ref[:, pair * LANES : (pair + 1) * LANES] = jnp.where(low, sides[0], sides[1]).astype(BF16)
    slot = lax.broadcasted_iota(jnp.int32, (heads, LANES), 1)
    mine = slot % heads == lax.broadcasted_iota(jnp.int32, (heads, LANES), 0)
    field = [mine & (slot // heads == i) for i in range(6)]
    for b in range(batch):
        value = jnp.zeros((heads, LANES), F32)
        for i, term in enumerate(split3(top[b]) + split3(total[b])):
            value = jnp.where(field[i], jnp.broadcast_to(term, (heads, LANES)), value)
        rows[b * heads : (b + 1) * heads, :] = value
    pick = lax.broadcasted_iota(jnp.int32, (batch, batch * heads), 1) // heads == lax.broadcasted_iota(
        jnp.int32, (batch, batch * heads), 0
    )
    stats = jnp.dot(
        jnp.where(pick, 1.0, 0.0).astype(BF16), rows[...].astype(BF16), preferred_element_type=F32
    )
    out_ref[:, heads * HEAD :] = stats.astype(BF16)
    for c in copies[4:]:
        c.wait()


def attention(queries, keys, values, lengths, weights):
    batch, _, width = keys.shape
    heads = queries.shape[1] // HEAD
    return pl.pallas_call(
        functools.partial(attention_body, heads, width // HEAD, len(weights)),
        out_shape=(
            pltpu.VMEM((batch, heads * HEAD + LANES), BF16),
            *(pltpu.VMEM(w.shape, w.dtype) for w in weights),
        ),
        in_specs=[HBM] * (4 + len(weights)),
        out_specs=(VMEM,) * (1 + len(weights)),
        scratch_shapes=[
            pltpu.SMEM(lengths.shape, jnp.int32),
            pltpu.VMEM(queries.shape, BF16),
            pltpu.VMEM(keys.shape, BF16),
            pltpu.VMEM(values.shape, BF16),
            pltpu.VMEM((batch * heads, LANES), F32),
            pltpu.SemaphoreType.DMA((4 + len(weights),)),
        ],
        compiler_params=LIMIT,
        name="attention",
    )(*map(off_chip, (lengths, queries, keys, values, *weights)))


def merge_body(heads, size, *refs):
    parts, weight, attended_ref, out_ref = refs[:size], refs[size], refs[size + 1], refs[size + 2]
    batch = parts[0].shape[0]
    tops, totals = [], []
    for part in parts:
        stats = part[:, heads * HEAD :].astype(F32)
        turned = [stats] + [pltpu.roll(stats, LANES - i * heads, 1) for i in range(1, 6)]
        tops.append(turned[0] + turned[1] + turned[2])
        totals.append(turned[3] + turned[4] + turned[5])
    top = pairwise(tops, jnp.maximum)
    shares = [jnp.exp(t - top) * s for t, s in zip(tops, totals)]
    inverse = 1.0 / pairwise(shares, add)
    shares = [s * inverse for s in shares]
    low = lax.broadcasted_iota(jnp.int32, (batch, LANES), 1) < HEAD
    wide = (batch, LANES)
    pieces = []
    for pair in range(heads // 2):
        columns = slice(pair * LANES, (pair + 1) * LANES)
        terms = []
        for share, part in zip(shares, parts):
            left = jnp.broadcast_to(share[:, 2 * pair : 2 * pair + 1], wide)
            right = jnp.broadcast_to(share[:, 2 * pair + 1 : 2 * pair + 2], wide)
            terms.append(jnp.where(low, left, right) * part[:, columns].astype(F32))
        piece = pairwise(terms, add)
        attended_ref[:, columns] = piece
        pieces.append(piece.astype(BF16))
    out_ref[...] = jnp.dot(jnp.concatenate(pieces, axis=1), weight[...], preferred_element_type=F32).astype(BF16)


def merge(parts, weight):
    batch = parts[0].shape[0]
    inputs, columns = weight.shape
    return pl.pallas_call(
        functools.partial(merge_body, inputs // HEAD, len(parts)),
        out_shape=(
            pltpu.VMEM((batch, inputs), F32),
            pltpu.VMEM((batch, columns), BF16),
        ),
        in_specs=[VMEM] * (len(parts) + 1),
        out_specs=(VMEM, VMEM),
        compiler_params=LIMIT,
        name="merge",
    )(*map(on_chip, (*parts, weight)))


def state_body(size, *refs):
    parts, residual, gain, state_ref, out_ref = refs[:size], *refs[size:]
    projected = pairwise([p[...].astype(F32) for p in parts], add)
    state = (projected + residual[...].astype(F32)).astype(BF16)
    state_ref[...] = state
    state = state.astype(F32)
    columns = state.shape[1]
    out_ref[:, :columns] = (state * gain[...].astype(F32).reshape(1, columns)).astype(BF16)
    squares = jnp.sum(state * state, axis=1, keepdims=True)
    lane = lax.broadcasted_iota(jnp.int32, (state.shape[0], LANES), 1)
    value = jnp.zeros(lane.shape, F32)
    for i, term in enumerate(split3(squares)):
        value = jnp.where(lane == i, jnp.broadcast_to(term, lane.shape), value)
    out_ref[:, columns:] = value.astype(BF16)


def state(parts, residual, gain):
    batch, columns = residual.shape
    return pl.pallas_call(
        functools.partial(state_body, len(parts)),
        out_shape=(
            pltpu.VMEM((batch, columns), BF16),
            pltpu.VMEM((batch, columns + LANES), BF16),
        ),
        in_specs=[VMEM] * (len(parts) + 2),
        out_specs=(VMEM, VMEM),
        compiler_params=LIMIT,
        name="state",
    )(*map(on_chip, (*parts, residual, gain)))


def expert_body(size, *refs):
    parts, (ids, probs, gate, up, down), outs = refs[:size], refs[size : size + 5], refs[size + 5 :]
    columns = outs[0].shape[1]
    me = lax.axis_index("kvp")
    held = gate.shape[0]
    squares = pairwise([jnp.sum(p[:, columns:].astype(F32), axis=1, keepdims=True) for p in parts], add)
    inverse = lax.rsqrt(squares / (columns * size) + EPSILON)
    sums = [0.0] * size
    for e in range(held):
        gate_sum, up_sum = 0.0, 0.0
        for s in range(size):
            rows = pl.ds(pl.multiple_of((me ^ s) * columns, LANES), columns)
            block = parts[s][:, :columns]
            gate_sum += jnp.dot(block, gate[e, rows, :], preferred_element_type=F32)
            up_sum += jnp.dot(block, up[e, rows, :], preferred_element_type=F32)
        gate_sum, up_sum = gate_sum * inverse, up_sum * inverse
        hidden = (gate_sum / (1.0 + jnp.exp(-gate_sum)) * up_sum).astype(BF16)
        chosen = ids[...] == me * held + e
        across = jnp.sum(jnp.where(chosen, probs[...], 0.0), axis=0, keepdims=True)
        batch = across.shape[1]
        own = lax.broadcasted_iota(jnp.int32, (batch, batch), 0) == lax.broadcasted_iota(
            jnp.int32, (batch, batch), 1
        )
        scale = jnp.sum(jnp.where(own, across, 0.0), axis=1, keepdims=True)
        for s in range(size):
            target = pl.ds(pl.multiple_of((me ^ s) * columns, LANES), columns)
            sums[s] += jnp.dot(hidden, down[e, :, target], preferred_element_type=F32) * scale
    for s in range(size):
        outs[s][...] = sums[s].astype(BF16)


def experts(parts, ids, probs, gate, up, down):
    size = len(parts)
    batch = parts[0].shape[0]
    columns = parts[0].shape[1] - LANES
    return pl.pallas_call(
        functools.partial(expert_body, size),
        out_shape=tuple(pltpu.VMEM((batch, columns), BF16) for _ in range(size)),
        in_specs=[VMEM] * (size + 5),
        out_specs=(VMEM,) * size,
        compiler_params=LIMIT,
        name="experts",
    )(*map(on_chip, (*parts, ids.T, probs.T, gate, up, down)))


def small_slice(
    queries, keys, values, lengths, out_weight, residual, norm_gain, expert_ids, gate_probs, w_gate, w_up, w_down
):
    block, out_weight, w_gate, w_up, w_down = attention(
        queries, keys, values, lengths, (out_weight, w_gate, w_up, w_down)
    )
    parts = share(block, "kvp")
    attended, projected = merge(parts, out_weight)
    own_state, message = state(share(projected, "tp"), residual, norm_gain)
    outputs = experts(share(message, "kvp"), expert_ids, gate_probs, w_gate, w_up, w_down)
    moved = exchange(outputs, "kvp")
    owned = pairwise([m.astype(F32) for m in moved], add).astype(BF16)
    moe_term = pairwise([m.astype(F32) for m in share(owned, "tp")], add)
    return attended, (own_state.astype(F32) + moe_term).astype(BF16)


def merged(part, axis, combine):
    gathered = jax.tree.map(lambda a: lax.all_gather(a, axis), part)

    def take(source):
        return jax.tree.map(lambda a: lax.dynamic_index_in_dim(a, source, 0, False), gathered)

    return lax.fori_loop(
        1, lax.axis_size(axis), lambda source, state: combine(state, take(source)), take(0)
    )


def slot_tables(expert_ids, gate_probs, experts, capacity):
    batch_size, top_count = expert_ids.shape
    flat_ids = expert_ids.reshape(-1)
    pair_count = flat_ids.shape[0]
    pair_order = jnp.arange(pair_count, dtype=jnp.int32)
    earlier_same = (flat_ids[:, None] == flat_ids[None, :]) & (
        pair_order[None, :] < pair_order[:, None]
    )
    slot_index = jnp.sum(earlier_same.astype(jnp.int32), axis=1)
    target_col = flat_ids * capacity + slot_index
    columns = jnp.arange(experts * capacity, dtype=jnp.int32)
    hit_table = (target_col[:, None] == columns[None, :]).astype(jnp.float32)
    hit_table = hit_table.reshape(batch_size, top_count, experts * capacity)
    dispatch = jnp.sum(hit_table, axis=1)
    combine = jnp.sum(hit_table * gate_probs[:, :, None], axis=1)
    return (dispatch, combine)


def merge_partial(earlier, latest):
    global_max = jnp.maximum(earlier[0], latest[0])
    lead_scale = jnp.exp(earlier[0] - global_max)
    trail_scale = jnp.exp(latest[0] - global_max)
    return (
        global_max,
        lead_scale * earlier[1] + trail_scale * latest[1],
        lead_scale[..., None] * earlier[2] + trail_scale[..., None] * latest[2],
    )


def large_slice(
    queries,
    keys,
    values,
    lengths,
    out_weight,
    residual,
    norm_gain,
    expert_ids,
    gate_probs,
    w_gate,
    w_up,
    w_down,
):
    batch_size = queries.shape[0]
    local_kv = keys.shape[2] // HEAD
    local_heads = queries.shape[1] // HEAD
    group_size = local_heads // local_kv
    ctx_dev = keys.shape[1]
    shards = lax.axis_size("kvp")
    query_heads = queries.reshape(batch_size, local_kv, group_size, HEAD)
    key_rows = keys.reshape(batch_size, ctx_dev, local_kv, HEAD)
    value_rows = values.reshape(batch_size, ctx_dev, local_kv, HEAD)
    scores = jnp.einsum(
        "bgrd,bcgd->bgrc", query_heads, key_rows, preferred_element_type=jnp.float32
    ) * HEAD ** (-0.5)
    position = lax.axis_index("kvp") * ctx_dev + jnp.arange(ctx_dev, dtype=jnp.int32)
    valid_key = (position[None, :] < lengths[:, None])[:, None, None, :]
    masked = jnp.where(valid_key, scores, NEGATIVE)
    block_max = jnp.max(masked, axis=3)
    weights = jnp.where(valid_key, jnp.exp(masked - block_max[..., None]), 0.0)
    rounded = weights.astype(jnp.bfloat16)
    block_sum = jnp.sum(rounded.astype(jnp.float32), axis=3)
    block_out = jnp.einsum(
        "bgrc,bcgd->bgrd", rounded, value_rows, preferred_element_type=jnp.float32
    )
    _, denominator, summed = merged(
        (block_max, block_sum, block_out), "kvp", merge_partial
    )
    attended = (summed / denominator[..., None]).reshape(batch_size, local_heads * HEAD)
    projected = lax.psum(
        jnp.dot(attended.astype(jnp.bfloat16), out_weight, preferred_element_type=jnp.float32), "tp"
    )
    hidden_state = lax.optimization_barrier(
        (projected + residual.astype(jnp.float32)).astype(jnp.bfloat16)
    )
    state_wide = hidden_state.astype(jnp.float32)
    col_count = hidden_state.shape[1]
    exp_dev = w_gate.shape[0]
    experts = exp_dev * shards
    capacity = min(batch_size, max(2, 2 * batch_size * expert_ids.shape[1] // experts))
    dispatch, combine = slot_tables(expert_ids, gate_probs, experts, capacity)
    total_sq = lax.psum(jnp.sum(state_wide * state_wide, axis=1), "kvp")
    inverse = lax.rsqrt(total_sq / (col_count * shards) + EPSILON)
    normed = (state_wide * inverse[:, None] * norm_gain.astype(jnp.float32)[None, :]).astype(
        jnp.bfloat16
    )
    outgoing = jnp.dot(
        dispatch.T.astype(jnp.bfloat16), normed, preferred_element_type=jnp.float32
    ).astype(jnp.bfloat16)
    outgoing = outgoing.reshape(experts, capacity, col_count)
    expert_rows = lax.all_to_all(outgoing, "kvp", split_axis=0, concat_axis=2, tiled=True)
    gate_proj = jnp.einsum("ecd,edf->ecf", expert_rows, w_gate, preferred_element_type=jnp.float32)
    up_proj = jnp.einsum("ecd,edf->ecf", expert_rows, w_up, preferred_element_type=jnp.float32)
    activation = (jax.nn.silu(gate_proj) * up_proj).astype(jnp.bfloat16)
    partial_value = jnp.einsum(
        "ecf,efd->ecd", activation, w_down, preferred_element_type=jnp.float32
    )
    returned = lax.all_to_all(partial_value, "kvp", split_axis=2, concat_axis=0, tiled=True)
    moe_local = jnp.dot(
        combine, returned.reshape(experts * capacity, col_count), precision=lax.Precision.HIGHEST
    )
    moe_term = lax.psum(moe_local, "tp")
    mixed = (state_wide + moe_term).astype(jnp.bfloat16)
    return (attended, mixed)


def on_device(queries, keys, values, lengths, out_weight, *rest):
    size, heads, kv = lax.axis_size("kvp"), queries.shape[1] // HEAD, keys.shape[2] // HEAD
    direct = (
        size in (2, 4, 8)
        and lax.axis_size("tp") in (2, 4, 8)
        and out_weight.shape[1] % LANES == 0
        and kv == 2
        and heads == 8 * kv
        and keys.shape[1] % LANES == 0
        and queries.shape[0] == 16
    )
    return (small_slice if direct else large_slice)(queries, keys, values, lengths, out_weight, *rest)


def solution(mesh):
    return jax.shard_map(
        on_device,
        mesh=mesh,
        in_specs=(
            P("grp", "tp"),
            P("grp", "kvp", "tp"),
            P("grp", "kvp", "tp"),
            P("grp"),
            P("tp", "kvp"),
            P("grp", "kvp"),
            P("kvp"),
            P("grp", None),
            P("grp", None),
            P("kvp", None, "tp"),
            P("kvp", None, "tp"),
            P("kvp", "tp", None),
        ),
        out_specs=(P("grp", "tp"), P("grp", "kvp")),
        check_vma=False,
    )
```
